1024 devices in a mesh: grp: 16 (over z_lo), cp: 64 (over y, x, z_hi, core).
Axes of the slice: x: 4, y: 4, z: 32 (z_hi: 2, z_lo: 16; z = z_hi * 16 + z_lo), core: 2. Of those that a mesh axis runs over, the one named last changes fastest.
Arguments:
- query_proj: bfloat16 [131072, 4096], P(('grp', 'cp')), may hold values from -6 to 6
- key_proj: bfloat16 [131072, 512], P(('grp', 'cp')), may hold values from -6 to 6
- value_projection: bfloat16 [131072, 512], P(('grp', 'cp')), may hold values from -6 to 6
- segment_ids: int32 [131072], P(('grp', 'cp')), may hold values from 0 to 511, never falling along the last dimension, each value on 1 to 1024 neighbouring positions
Outputs:
- attended: bfloat16 [131072, 4096], P(('grp', 'cp'))
The draws below stay inside these ranges and needn't reach their ends.
Inputs may be any that keep to these rules, and one draw needn't show every extreme that they name: `segment_ids`: never falls along the stream; every document has 1 to 1024 tokens, and one has exactly 1024.
All inputs are finite; a program needn't handle non-finite values.
Results may differ from the reference program's by a relative error of at most 0.0034.
Values may be sent and summed in bfloat16 or wider, within the bound.
No kernel may reach another device: no remote copies, remote signals or barrier semaphores. Data moves between devices by JAX's collectives and lax.ppermute only.
A program may use at most 64 MiB of HBM per device.

```python
import math
import jax
import jax.numpy as jnp
import numpy as np
from jax import lax

QUERY_HEADS = 32
KEY_VALUE_HEADS = 4
HEAD_WIDTH = 128
TOK_DEV = 128
SPAN = 8
MOST = 1024
STREAM_TOKENS = 131072
DOCS = 512


def draw_query_proj(key, part):
    unmasked_result = jnp.clip(jax.random.normal(jax.random.fold_in(key, 11), (STREAM_TOKENS, QUERY_HEADS * HEAD_WIDTH), jnp.float32), -6.0, 6.0)
    return unmasked_result.astype(jnp.bfloat16)


def draw_key_proj(key, part):
    unmasked_result = jnp.clip(jax.random.normal(jax.random.fold_in(key, 12), (STREAM_TOKENS, KEY_VALUE_HEADS * HEAD_WIDTH), jnp.float32), -6.0, 6.0)
    return unmasked_result.astype(jnp.bfloat16)


def levels(rng, dims, split, smallest, high):
    loudness = 1.0
    for dim, blocks in split:
        steps = jax.random.uniform(jax.random.fold_in(jax.random.fold_in(rng, 6), dim), (blocks,), jnp.float32, smallest / len(split), high / len(split))
        loudness = loudness * jnp.repeat(jnp.exp(steps), dims[dim] // blocks).reshape((-1,) + (1,) * (len(dims) - 1 - dim))
    return loudness


def profile(count, total, bound, skew):
    portions = [(1 << 20) // math.isqrt(rank ** skew) + 1 for rank in range(2, count + 1)]
    spare, counts = total - bound - (count - 1), [1] * (count - 1)
    while spare > 0:
        candidates = [i for i in range(count - 1) if counts[i] < bound]
        whole, budget = sum([portions[i] for i in candidates]), spare
        for i in candidates:
            addition = min(bound - counts[i], max(1, budget * portions[i] // whole), spare)
            counts[i] = counts[i] + addition
            spare = spare - addition
    return np.array([bound] + counts)


def ragged(own_key, amount, total, reach, lean):
    if amount == 2:
        one = jax.random.randint(own_key, (), max(1, total - reach), min(reach, total - 1) + 1)
        return jnp.stack([one, total - one])
    lengths = jnp.asarray(profile(amount, total, reach, lean), jnp.int32)
    twos = (amount - 1) // 2
    giver, taker = lengths[1:1 + 2 * twos:2], lengths[2:2 + 2 * twos:2]
    slack = jnp.minimum(giver - 1, reach - taker)
    moved = jax.random.randint(jax.random.fold_in(own_key, 1), (twos,), 0, 1 << 20) % (slack + 1)
    lengths = lengths.at[1:1 + 2 * twos:2].set(giver - moved).at[2:2 + 2 * twos:2].set(taker + moved)
    return lengths[jax.random.permutation(jax.random.fold_in(own_key, 2), amount)]


def scatter_about(stream_key, dims, spread, reach, pieces=(), kind=jnp.bfloat16):
    gain = levels(stream_key, dims, pieces, -0.22, 0.18) if pieces else 1.0
    result = jax.random.normal(stream_key, dims, jnp.float32) * spread * gain
    return jnp.minimum(jnp.maximum(result, -reach), reach).astype(kind)


def setup_inputs(seed: int = 0) -> dict:
    key_list = jax.random.split(jax.random.key(seed), 5)
    return {
        "query_proj": draw_query_proj(jax.random.fold_in(key_list[4], 71), 0),
        "key_proj": draw_key_proj(jax.random.fold_in(key_list[4], 71), 0),
        "value_projection": scatter_about(key_list[2], (STREAM_TOKENS, KEY_VALUE_HEADS * HEAD_WIDTH), 1.0, 6.0, ((0, 1024),)),
        "segment_ids": jnp.searchsorted(jnp.cumsum(ragged(key_list[3], DOCS, STREAM_TOKENS, MOST, 2)), jnp.arange(STREAM_TOKENS), side="right").astype(jnp.int32),
    }


def attend_window(query_rows, key_win, value_win, seg_query, seg_keys, pos_query, pos_keys):
    tok_rows = query_rows.shape[0]
    group_size = query_rows.shape[1] // key_win.shape[1]
    kv_count = key_win.shape[1] // HEAD_WIDTH
    score_scale = 1.0 / math.sqrt(HEAD_WIDTH)
    visible = (seg_query[:, None] == seg_keys[None, :]) & (pos_keys[None, :] <= pos_query[:, None]) & (pos_keys[None, :] >= 0)
    pieces_out = []
    for kv_head in range(kv_count):
        q_block = query_rows[:, kv_head * group_size * HEAD_WIDTH:(kv_head + 1) * group_size * HEAD_WIDTH].reshape(tok_rows, group_size, HEAD_WIDTH).astype(jnp.float32)
        k_block = key_win[:, kv_head * HEAD_WIDTH:(kv_head + 1) * HEAD_WIDTH].astype(jnp.float32)
        v_block = value_win[:, kv_head * HEAD_WIDTH:(kv_head + 1) * HEAD_WIDTH].astype(jnp.float32)
        scores = jnp.einsum('tgd,sd->tgs', q_block, k_block, precision=lax.Precision.HIGHEST) * score_scale
        scores = jnp.where(visible[:, None, :], scores, -jnp.inf)
        row_max = lax.optimization_barrier(jnp.max(scores, axis=2, keepdims=True))
        weights = jnp.exp(scores - row_max)
        row_total = lax.optimization_barrier(jnp.sum(weights, axis=2, keepdims=True))
        probs = lax.optimization_barrier(weights.astype(jnp.bfloat16)).astype(jnp.float32)
        mixed = jnp.einsum('tgs,sd->tgd', probs, v_block, precision=lax.Precision.HIGHEST) / row_total
        pieces_out.append(mixed.reshape(tok_rows, group_size * HEAD_WIDTH).astype(jnp.bfloat16))
    return jnp.concatenate(pieces_out, axis=1)

def reference(query_proj, key_proj, value_projection, segment_ids):
    margin = SPAN * TOK_DEV
    padded_keys = jnp.concatenate([jnp.zeros((margin, key_proj.shape[1]), key_proj.dtype), key_proj], 0)
    padded_values = jnp.concatenate([jnp.zeros((margin, value_projection.shape[1]), value_projection.dtype), value_projection], 0)
    padded_segs = jnp.concatenate([jnp.full((margin,), -1, jnp.int32), segment_ids.astype(jnp.int32)], 0)
    block_count = STREAM_TOKENS // TOK_DEV

    def one_block(block_index):
        first_pos = (block_index * TOK_DEV).astype(jnp.int32)
        query_rows = lax.dynamic_slice_in_dim(query_proj, first_pos, TOK_DEV, 0)
        seg_query = lax.dynamic_slice_in_dim(segment_ids.astype(jnp.int32), first_pos, TOK_DEV, 0)
        key_win = lax.dynamic_slice_in_dim(padded_keys, first_pos, margin + TOK_DEV, 0)
        value_win = lax.dynamic_slice_in_dim(padded_values, first_pos, margin + TOK_DEV, 0)
        seg_keys = lax.dynamic_slice_in_dim(padded_segs, first_pos, margin + TOK_DEV, 0)
        pos_query = first_pos + jnp.arange(TOK_DEV, dtype=jnp.int32)
        pos_keys = first_pos - margin + jnp.arange(margin + TOK_DEV, dtype=jnp.int32)
        return attend_window(query_rows, key_win, value_win, seg_query, seg_keys, pos_query, pos_keys)
    blocks_out = lax.map(one_block, jnp.arange(block_count, dtype=jnp.int32))
    return blocks_out.reshape(STREAM_TOKENS, QUERY_HEADS * HEAD_WIDTH)
```

```python
import functools
import math

import jax
import jax.numpy as jnp
from jax import lax
from jax.experimental import pallas as pl
from jax.experimental.pallas import tpu as pltpu
from jax.sharding import PartitionSpec as P

HEAD = 128
META = 8
AXES = ("grp", "cp")
HIDDEN = -1e30
STACK = 4


def moved(value, target):
    count = lax.axis_size(AXES)
    pairs = [(s, target(s)) for s in range(count)]
    return lax.ppermute(value, AXES, [(s, t) for s, t in pairs if t is not None and 0 <= t < count])


def doc_rows(segments, width):
    ids = (segments + 1)[None, :]
    row = lax.broadcasted_iota(jnp.int32, (META, ids.shape[1]), 0)
    digits = jnp.where(row == 0, ids // 256, jnp.where(row == 1, ids % 256, 0)).astype(jnp.bfloat16)
    return jnp.pad(digits, ((0, 0), (0, width - digits.shape[1])))


def doc_line(rows):
    return rows[0:1, :].astype(jnp.float32) * 256.0 + rows[1:2, :].astype(jnp.float32)


def attend(heads, q_ref, own_docs, packs, docs, before, outs):
    tok = q_ref.shape[0]
    mine = jnp.broadcast_to(own_docs, (tok, tok)).T
    tiles = [mine == jnp.broadcast_to(d, (tok, tok)) for d in docs]
    if not before:
        rows = lax.broadcasted_iota(jnp.int32, (tok, tok), 0)
        cols = lax.broadcasted_iota(jnp.int32, (tok, tok), 1)
        tiles[0] = tiles[0] & (cols <= rows)
    mask = jnp.concatenate([jnp.concatenate(tiles, 1)] * STACK, 0)
    keys = jnp.concatenate([p[0:tok, :] for p in packs], 0)
    values = jnp.concatenate([p[tok : 2 * tok, :] for p in packs], 0)
    to_base_two = math.log2(math.e) / math.sqrt(HEAD)
    full = (STACK * tok, HEAD)
    for start in range(0, heads, STACK):
        rows = slice(start * tok, (start + STACK) * tok)
        queries = jnp.concatenate([q_ref[:, i * HEAD : (i + 1) * HEAD] for i in range(start, start + STACK)], 0)
        scores = lax.dot_general(queries, keys, (((1,), (1,)), ((), ())), preferred_element_type=jnp.float32)
        scores = jnp.where(mask, scores * to_base_two, HIDDEN)
        top = jnp.broadcast_to(jnp.max(scores, axis=1, keepdims=True), full)
        if before:
            old = before[1][0, rows, :]
            top = jnp.maximum(top, old)
        weights = jnp.exp2(scores - jnp.concatenate([top] * len(packs), 1))
        total = jnp.broadcast_to(jnp.sum(weights, axis=1, keepdims=True), full)
        mixed = jnp.dot(weights.astype(jnp.bfloat16), values, preferred_element_type=jnp.float32)
        if before:
            share = jnp.exp2(old - top)
            mixed = (mixed + before[0][0, rows, :] * share) * (1.0 / (total + share))
            for i in range(STACK):
                outs[0][:, (start + i) * HEAD : (start + i + 1) * HEAD] = mixed[i * tok : (i + 1) * tok].astype(jnp.bfloat16)
        else:
            outs[0][0, rows, :] = mixed * (1.0 / total)
            outs[1][0, rows, :] = top + jnp.log2(total)


def near_kernel(heads, q, p0, p1, p2, p3, p4, d0, d1, d2, d3, d4, *outs):
    docs = [doc_line(d[...]) for d in (d0, d1, d2, d3, d4)]
    attend(heads, q, docs[0], [p[...] for p in (p0, p1, p2, p3, p4)], docs, (), outs)


def far_kernel(heads, flag, q, own, p0, right, p1, p2, p3, d0, d_right, d1, d2, d3, mixed, logs, *outs):
    put_right = flag[0] > 0
    docs = [jnp.where(put_right, doc_line(d_right[...]), doc_line(d0[...]))] + [doc_line(d[...]) for d in (d1, d2, d3)]
    packs = [jnp.where(put_right, right[...], p0[...])] + [p[...] for p in (p1, p2, p3)]
    attend(heads, q, doc_line(own[...]), packs, docs, (mixed, logs), outs)


def shards(query_proj, key_proj, value_projection, segment_ids):
    tok, width = query_proj.shape
    kv = key_proj.shape[1] // HEAD
    heads = width // HEAD // kv
    group = lax.axis_size("cp")
    place = lax.axis_index("cp")
    odd = place % 2 == 1
    opening = place < 4
    closing = place >= group - 4
    partner = lambda s: s ^ 1

    own = jnp.concatenate([key_proj, value_projection, doc_rows(segment_ids, key_proj.shape[1])], 0)

    def over(s):
        return s + 4 if s % group >= group - 4 else s + 4 + group if s % group >= group - 8 else None

    outside = moved(own, over)
    crossed = moved(own, lambda s: s // group * group + (s + 2) % group)
    round_four = moved(jnp.where(closing, outside, own), lambda s: s // group * group + (s + 4) % group)
    four = jnp.where(opening, outside, round_four)
    eight = moved(four, lambda s: s + 4 if s % group < group - 4 else None)
    eight = jnp.where(opening, round_four, eight)
    four_there = moved(four, partner)
    rest_there = moved(jnp.where(odd, eight, own), partner)
    near = [own, four, eight, four_there, rest_there]

    tall = jax.ShapeDtypeStruct((kv, heads * tok, HEAD), jnp.float32)
    slab = pl.BlockSpec((1, heads * tok, HEAD), lambda h: (h, 0, 0))
    pack = pl.BlockSpec((2 * tok + META, HEAD), lambda h: (0, h))
    docs = pl.BlockSpec((META, HEAD), lambda h: (2 * tok // META, 0))
    query = pl.BlockSpec((tok, heads * HEAD), lambda h: (0, h))
    flag = pl.BlockSpec(memory_space=pltpu.SMEM)

    def call(kernel, shard_count, in_specs, final=False):
        return pl.pallas_call(
            functools.partial(kernel, heads),
            grid=(kv,),
            in_specs=in_specs,
            out_specs=query if final else [slab] * 2,
            out_shape=jax.ShapeDtypeStruct((tok, width), jnp.bfloat16) if final else [tall] * 2,
            compiler_params=pltpu.CompilerParams(dimension_semantics=("arbitrary",), vmem_limit_bytes=20 << 20),
            cost_estimate=pl.CostEstimate(
                flops=shard_count * 4 * tok * tok * HEAD * heads * kv, bytes_accessed=9 << 20, transcendentals=0
            ),
        )

    mixed, logs = call(near_kernel, 5, [query] + [pack] * 5 + [docs] * 5)(query_proj, *near, *near)

    turned = lambda s: group if s % group < 2 else 0
    crossed, mixed, logs, query_late, own_late = lax.optimization_barrier((crossed, mixed, logs, query_proj, own))
    onward = moved(crossed, lambda s: s + 4 + turned(s))
    put_right = moved(crossed, lambda s: s + group if s % group < 2 else None)
    crossed_there = moved(crossed, lambda s: (s ^ 1) + turned(s))
    onward_there = moved(onward, partner)
    first = (place < 2).astype(jnp.int32).reshape(1)
    far = [crossed, put_right, crossed_there, onward, onward_there]
    return call(far_kernel, 4, [flag, query, docs] + [pack] * 5 + [docs] * 5 + [slab] * 2, True)(
        first, query_late, own_late, *far, *far, mixed, logs
    )


def solution(mesh):
    return jax.shard_map(
        shards,
        mesh=mesh,
        in_specs=(P(AXES, None), P(AXES, None), P(AXES, None), P(AXES)),
        out_specs=P(AXES, None),
        check_vma=False,
    )
```

```python
import functools
import math

import jax
import jax.numpy as jnp
from jax import lax
from jax.experimental import pallas as pl
from jax.experimental.pallas import tpu as pltpu
from jax.sharding import PartitionSpec as P

HEAD = 128
META = 8
AXES = ("grp", "cp")
HIDDEN = -1e30
STACK = 4


def moved(value, target):
    count = lax.axis_size(AXES)
    pairs = [(s, target(s)) for s in range(count)]
    return lax.ppermute(value, AXES, [(s, t) for s, t in pairs if t is not None and 0 <= t < count])


def doc_rows(segments, width):
    ids = (segments + 1)[None, :]
    row = lax.broadcasted_iota(jnp.int32, (META, ids.shape[1]), 0)
    digits = jnp.where(row == 0, ids // 256, jnp.where(row == 1, ids % 256, 0)).astype(jnp.bfloat16)
    return jnp.pad(digits, ((0, 0), (0, width - digits.shape[1])))


def doc_line(rows):
    return rows[0:1, :].astype(jnp.float32) * 256.0 + rows[1:2, :].astype(jnp.float32)


def attend(heads, q_ref, own_docs, packs, docs, before, outs):
    tok = q_ref.shape[0]
    mine = jnp.broadcast_to(own_docs, (tok, tok)).T
    tiles = [mine == jnp.broadcast_to(d, (tok, tok)) for d in docs]
    if not before:
        rows = lax.broadcasted_iota(jnp.int32, (tok, tok), 0)
        cols = lax.broadcasted_iota(jnp.int32, (tok, tok), 1)
        tiles[0] = tiles[0] & (cols <= rows)
    mask = jnp.concatenate([jnp.concatenate(tiles, 1)] * STACK, 0)
    keys = jnp.concatenate([p[0:tok, :] for p in packs], 0)
    values = jnp.concatenate([p[tok : 2 * tok, :] for p in packs], 0)
    to_base_two = math.log2(math.e) / math.sqrt(HEAD)
    full = (STACK * tok, HEAD)
    for start in range(0, heads, STACK):
        rows = slice(start * tok, (start + STACK) * tok)
        queries = jnp.concatenate([q_ref[:, i * HEAD : (i + 1) * HEAD] for i in range(start, start + STACK)], 0)
        scores = lax.dot_general(queries, keys, (((1,), (1,)), ((), ())), preferred_element_type=jnp.float32)
        scores = jnp.where(mask, scores * to_base_two, HIDDEN)
        top = jnp.broadcast_to(jnp.max(scores, axis=1, keepdims=True), full)
        if before:
            old = before[1][0, rows, :]
            top = jnp.maximum(top, old)
        weights = jnp.exp2(scores - jnp.concatenate([top] * len(packs), 1))
        total = jnp.broadcast_to(jnp.sum(weights, axis=1, keepdims=True), full)
        mixed = jnp.dot(weights.astype(jnp.bfloat16), values, preferred_element_type=jnp.float32)
        if before:
            share = jnp.exp2(old - top)
            mixed = (mixed + before[0][0, rows, :] * share) * (1.0 / (total + share))
            for i in range(STACK):
                outs[0][:, (start + i) * HEAD : (start + i + 1) * HEAD] = mixed[i * tok : (i + 1) * tok].astype(jnp.bfloat16)
        else:
            outs[0][0, rows, :] = mixed * (1.0 / total)
            outs[1][0, rows, :] = top + jnp.log2(total)


def near_kernel(heads, q, p0, p1, p2, p3, p4, d0, d1, d2, d3, d4, *outs):
    docs = [doc_line(d[...]) for d in (d0, d1, d2, d3, d4)]
    attend(heads, q, docs[0], [p[...] for p in (p0, p1, p2, p3, p4)], docs, (), outs)


def far_kernel(heads, q, own, p0, p1, p2, p3, d0, d1, d2, d3, mixed, logs, *outs):
    docs = [doc_line(d[...]) for d in (d0, d1, d2, d3)]
    attend(heads, q, doc_line(own[...]), [p[...] for p in (p0, p1, p2, p3)], docs, (mixed, logs), outs)


def shards(query_proj, key_proj, value_projection, segment_ids):
    tok, width = query_proj.shape
    kv = key_proj.shape[1] // HEAD
    heads = width // HEAD // kv
    group = lax.axis_size("cp")
    place = lax.axis_index("cp")
    odd = place % 2 == 1
    opening = place < 4
    closing = place >= group - 4
    partner = lambda s: s ^ 1

    own = jnp.concatenate([key_proj, value_projection, doc_rows(segment_ids, key_proj.shape[1])], 0)

    def over(s):
        return s + 4 if s % group >= group - 4 else s + 4 + group if s % group >= group - 8 else None

    outside = moved(own, over)
    crossed = moved(own, lambda s: s // group * group + (s + 2) % group)
    round_four = moved(jnp.where(closing, outside, own), lambda s: s // group * group + (s + 4) % group)
    four = jnp.where(opening, outside, round_four)
    eight = moved(four, lambda s: s + 4 if s % group < group - 4 else None)
    eight = jnp.where(opening, round_four, eight)
    four_there = moved(four, partner)
    rest_there = moved(jnp.where(odd, eight, own), partner)
    near = [own, four, eight, four_there, rest_there]

    tall = jax.ShapeDtypeStruct((kv, heads * tok, HEAD), jnp.float32)
    slab = pl.BlockSpec((1, heads * tok, HEAD), lambda h: (h, 0, 0))
    pack = pl.BlockSpec((2 * tok + META, HEAD), lambda h: (0, h))
    docs = pl.BlockSpec((META, HEAD), lambda h: (2 * tok // META, 0))
    query = pl.BlockSpec((tok, heads * HEAD), lambda h: (0, h))
    flag = pl.BlockSpec(memory_space=pltpu.SMEM)

    def call(kernel, shard_count, in_specs, final=False):
        return pl.pallas_call(
            functools.partial(kernel, heads),
            grid=(kv,),
            in_specs=in_specs,
            out_specs=query if final else [slab] * 2,
            out_shape=jax.ShapeDtypeStruct((tok, width), jnp.bfloat16) if final else [tall] * 2,
            compiler_params=pltpu.CompilerParams(dimension_semantics=("arbitrary",), vmem_limit_bytes=20 << 20),
            cost_estimate=pl.CostEstimate(
                flops=shard_count * 4 * tok * tok * HEAD * heads * kv, bytes_accessed=9 << 20, transcendentals=0
            ),
        )

    mixed, logs = call(near_kernel, 5, [query] + [pack] * 5 + [docs] * 5)(query_proj, *near, *near)

    crossed, mixed = lax.optimization_barrier((crossed, mixed))
    onward = moved(crossed, lambda s: s + 4 + (group if s % group < 2 else 0))
    put_right = moved(crossed, lambda s: s + group if s % group < 2 else None)
    crossed = jnp.where(place < 2, put_right, crossed)
    crossed_there = moved(crossed, partner)
    onward_there = moved(onward, partner)
    far = [crossed, crossed_there, onward, onward_there]
    return call(far_kernel, 4, [query, docs] + [pack] * 4 + [docs] * 4 + [slab] * 2, True)(
        query_proj, own, *far, *far, mixed, logs
    )


def solution(mesh):
    return jax.shard_map(
        shards,
        mesh=mesh,
        in_specs=(P(AXES, None), P(AXES, None), P(AXES, None), P(AXES)),
        out_specs=P(AXES, None),
        check_vma=False,
    )
```
